32 devices in a mesh: gx: 8 (over z, core), gy: 4 (over y, x).
Axes of the slice: x: 2, y: 2, z: 4, core: 2. Of those that a mesh axis runs over, the one named last changes fastest.
Arguments:
- density: float32 [512, 512, 512], P('gx', 'gy'), may hold values from -6 to 6
- radius_cells: int32 [2], replicated, may hold values from 1 to 32
Outputs:
- filtered: float32 [2, 512, 512, 512], P(None, 'gx', 'gy')
The draws below stay inside these ranges and needn't reach their ends.
All inputs are finite; a program needn't handle non-finite values.
Results may differ from the reference program's by a relative error of at most 0.0001.
Values sent between devices are 32-bit elements; how exact they have to be, the bound alone decides.
A program may use at most 192 MiB of HBM per device.

```python
import math
import jax
import jax.numpy as jnp

N = 512
RADII = 2


def block_scale(rng, dims, cuts, low, largest):
    gain = 1.0
    for dim, blocks in cuts:
        heights = jax.random.uniform(jax.random.fold_in(jax.random.fold_in(rng, 6), dim), (blocks,), jnp.float32, low / len(cuts), largest / len(cuts))
        gain = gain * jnp.repeat(jnp.exp(heights), dims[dim] // blocks).reshape((-1,) + (1,) * (len(dims) - 1 - dim))
    return gain


def normal_values(stream_key, shape, deviation, most, split=(), kind=jnp.bfloat16):
    level = block_scale(stream_key, shape, split, -0.22, 0.18) if split else 1.0
    values = jax.random.normal(stream_key, shape, jnp.float32) * deviation * level
    return jnp.minimum(jnp.maximum(values, -most), most).astype(kind)


def setup_inputs(seed: int = 0) -> dict:
    keys = jax.random.split(jax.random.key(seed), 3)
    density = normal_values(keys[0], (N, N, N), 1.0, 6.0, ((0, 8), (1, 4)), jnp.float32)
    radius_cells = jax.random.randint(keys[1], (RADII,), 1, 33).astype(jnp.int32)
    return {"density": density, "radius_cells": radius_cells}


def window(u_value):
    is_small = u_value < 0.2
    safe_u = jnp.where(is_small, 1.0, u_value)
    closed_form = 3.0 * (jnp.sin(safe_u) - safe_u * jnp.cos(safe_u)) / (safe_u * safe_u * safe_u)
    series = 1.0 - u_value * u_value / 10.0 + u_value ** 4 / 280.0
    return jnp.where(is_small, series, closed_form)

def reference(density, radius_cells):
    spectrum = jnp.fft.fftn(density)
    indices = jnp.arange(N, dtype=jnp.int32)
    signed = jnp.where(indices > N // 2, indices - N, indices).astype(jnp.float32)
    squares = signed * signed
    k_squared = squares[:, None, None] + squares[None, :, None] + squares[None, None, :]
    k_length = 2.0 * math.pi / N * jnp.sqrt(k_squared)
    results = []
    for radius_index in range(RADII):
        weights = window(k_length * radius_cells[radius_index].astype(jnp.float32))
        results.append(jnp.real(jnp.fft.ifftn(spectrum * weights)).astype(jnp.float32))
    return jnp.stack(results)
```

```python
import functools
import math

import jax
import jax.numpy as jnp
import numpy as np
from jax import lax
from jax.experimental import pallas as pl
from jax.experimental.pallas import tpu as pltpu
from jax.sharding import PartitionSpec as P

MESH = pl.DeviceIdType.MESH
STEP = 8
PIECE = 16
VMEM = 63 * 1024 * 1024


def window(k_squared, scale_squared):
    u_squared = k_squared * scale_squared
    u_value = jnp.sqrt(u_squared)
    is_small = u_value < 0.2
    safe = jnp.where(is_small, 1.0, u_value)
    turns = jnp.floor(safe * (1.0 / math.pi) + 0.5)
    rest = safe - turns * 3.140625
    rest = rest - turns * 9.67502593994140625e-4
    rest = rest - turns * 1.509957990978376432e-7
    s2 = rest * rest
    sin_v = rest * (1.0 + s2 * (-1.6666666666e-1 + s2 * (8.3333333e-3 + s2 * (
        -1.98412698e-4 + s2 * (2.75573192e-6 + s2 * -2.50521084e-8)))))
    cos_v = 1.0 + s2 * (-0.5 + s2 * (4.16666666e-2 + s2 * (-1.38888889e-3 + s2 * (
        2.48015873e-5 + s2 * (-2.75573192e-7 + s2 * 2.08767570e-9)))))
    half = turns * 0.5
    sign = jnp.where(half == jnp.floor(half), 3.0, -3.0)
    closed = sign * (sin_v - safe * cos_v) / (safe * safe * safe)
    series = 1.0 - u_squared / 10.0 + u_squared * u_squared / 280.0
    return jnp.where(is_small, series, closed)


def basis(length, order):
    freq = np.array([length // 2 if s and f == 0 else f for f, s in order])
    sine = np.array([s and f > 0 for f, s in order])
    angle = 2.0 * math.pi / length * (np.outer(freq, np.arange(length)) % length)
    table = np.where(sine[:, None], np.sin(angle), np.cos(angle))
    gain = np.where((freq == 0) | (freq == length // 2), 1.0, 2.0) / length
    return table, gain[:, None]


def blocked(length, parts):
    width = length // 2 // parts
    return [(p * width + j, s) for p in range(parts) for s in (0, 1) for j in range(width)]


def paired(length):
    return [(f, s) for f in range(length // 2) for s in (0, 1)]


def tripled(table, axis):
    table = jnp.asarray(table, jnp.float32)
    high = table.astype(jnp.bfloat16)
    low = (table - high.astype(jnp.float32)).astype(jnp.bfloat16)
    return jnp.concatenate([high, low, high], axis)


def split(values, axis):
    high = values.astype(jnp.bfloat16)
    low = (values - high.astype(jnp.float32)).astype(jnp.bfloat16)
    return jnp.concatenate([high, high, low], axis)


def product(matrix, columns):
    width = columns[0].shape[1]
    if width % 128:
        return [jnp.dot(matrix, split(c, 0), preferred_element_type=jnp.float32) for c in columns]
    out = jnp.dot(matrix, split(jnp.concatenate(columns, 1), 0), preferred_element_type=jnp.float32)
    return [out[:, i * width:(i + 1) * width] for i in range(len(columns))]


def greet(count_gx, count_gy, me, my):
    barrier = pltpu.get_barrier_semaphore()
    for s in range(1, count_gx):
        pl.semaphore_signal(barrier, inc=1, device_id={"gx": lax.rem(me + s, count_gx)}, device_id_type=MESH)
    for s in range(1, count_gy):
        pl.semaphore_signal(barrier, inc=1, device_id={"gy": lax.rem(my + s, count_gy)}, device_id_type=MESH)
    pl.semaphore_wait(barrier, count_gx + count_gy - 2)


def forward_kernel(count_gx, count_gy, density, fwd_z, fwd_y, cube, loaded, packed, lines, planes,
                   load_sem, z_send, z_recv, x_send, x_recv):
    rows_x, rows_y, length = density.shape
    lanes = length // count_gy
    cols = length // count_gx
    steps = rows_x // STEP
    me, my = lax.axis_index("gx"), lax.axis_index("gy")

    def load(i):
        return pltpu.make_async_copy(
            density.at[pl.ds(i * STEP, STEP)], loaded.at[lax.rem(i, 2)], load_sem.at[lax.rem(i, 2)])

    def z_part(i, s, source):
        return pltpu.make_async_remote_copy(
            src_ref=packed.at[i, lax.rem(my + s, count_gy)],
            dst_ref=lines.at[pl.ds(i * STEP, STEP), pl.ds(source * rows_y, rows_y)],
            send_sem=z_send.at[i, s], recv_sem=z_recv.at[i, s],
            device_id={"gy": lax.rem(my + s, count_gy)}, device_id_type=MESH)

    def z_own(i):
        return pltpu.make_async_copy(
            packed.at[i, my], lines.at[pl.ds(i * STEP, STEP), pl.ds(my * rows_y, rows_y)], z_send.at[i, 0])

    def x_part(i, s, source):
        return pltpu.make_async_remote_copy(
            src_ref=planes.at[pl.ds(i * STEP, STEP), pl.ds(lax.rem(me + s, count_gx) * cols, cols)],
            dst_ref=cube.at[pl.ds(source * rows_x + i * STEP, STEP)],
            send_sem=x_send.at[i, s], recv_sem=x_recv.at[i, s],
            device_id={"gx": lax.rem(me + s, count_gx)}, device_id_type=MESH)

    def x_own(i):
        return pltpu.make_async_copy(
            planes.at[pl.ds(i * STEP, STEP), pl.ds(me * cols, cols)],
            cube.at[pl.ds(me * rows_x + i * STEP, STEP)], x_send.at[i, 0])

    load(0).start()
    greet(count_gx, count_gy, me, my)

    def along_z(i, _):
        @pl.when(i + 1 < steps)
        def _():
            load(i + 1).start()
        load(i).wait()

        def pair(j, _):
            rows = loaded[lax.rem(i, 2), pl.ds(2 * j, 2)].reshape(2 * rows_y, length)
            out = jnp.dot(split(rows, 1), fwd_z[...], preferred_element_type=jnp.float32)
            for b in range(count_gy):
                packed[i, b, pl.ds(2 * j, 2)] = out[:, b * lanes:(b + 1) * lanes].reshape(2, rows_y, lanes)
            return 0

        lax.fori_loop(0, STEP // 2, pair, 0)
        for s in range(1, count_gy):
            z_part(i, s, my).start()
        z_own(i).start()
        return 0

    lax.fori_loop(0, steps, along_z, 0)

    def along_y(i, _):
        for s in range(1, count_gy):
            z_part(i, s, lax.rem(my + count_gy - s, count_gy)).wait_recv()
        z_own(i).wait()

        def pair(j, _):
            row = i * STEP + 2 * j
            out = product(fwd_y[...], [lines[row], lines[row + 1]])
            planes[row] = out[0]
            planes[row + 1] = out[1]
            return 0

        lax.fori_loop(0, STEP // 2, pair, 0)
        for s in range(1, count_gx):
            x_part(i, s, me).start()
        x_own(i).start()
        return 0

    lax.fori_loop(0, steps, along_y, 0)

    def finish(i, _):
        for s in range(1, count_gy):
            z_part(i, s, my).wait_send()
        for s in range(1, count_gx):
            x_part(i, s, me).wait_send()
            x_part(i, s, lax.rem(me + count_gx - s, count_gx)).wait_recv()
        x_own(i).wait()
        return 0

    lax.fori_loop(0, steps, finish, 0)


def inverse_kernel(count_gx, count_gy, rows_x, rows_y, scales, cube, fwd_x, inv_x, inv_y,
                   early, late, result, loaded, first, second, lines, planes,
                   load_sem, a_send, a_recv, b_send, b_recv, line_sem, z_send, z_recv):
    length, cols, lanes = cube.shape
    pieces = cols // PIECE
    steps = rows_x // STEP
    mid = length // 2
    me, my = lax.axis_index("gx"), lax.axis_index("gy")
    slots = planes.shape[0]

    def load(c):
        return pltpu.make_async_copy(
            cube.at[:, pl.ds(c * PIECE, PIECE)], loaded.at[lax.rem(c, 2)], load_sem.at[lax.rem(c, 2)])

    def a_part(c, s, source):
        return pltpu.make_async_remote_copy(
            src_ref=first.at[c, pl.ds(lax.rem(me + s, count_gx) * rows_x, rows_x)],
            dst_ref=early.at[:, pl.ds(source * cols + c * PIECE, PIECE)],
            send_sem=a_send.at[c, s], recv_sem=a_recv.at[c, s],
            device_id={"gx": lax.rem(me + s, count_gx)}, device_id_type=MESH)

    def a_own(c):
        return pltpu.make_async_copy(
            first.at[c, pl.ds(me * rows_x, rows_x)],
            early.at[:, pl.ds(me * cols + c * PIECE, PIECE)], a_send.at[c, 0])

    def b_part(i, s, source):
        return pltpu.make_async_remote_copy(
            src_ref=second.at[pl.ds(lax.rem(me + s, count_gx) * rows_x + i * STEP, STEP)],
            dst_ref=late.at[pl.ds(i * STEP, STEP), pl.ds(source * cols, cols)],
            send_sem=b_send.at[i, s], recv_sem=b_recv.at[i, s],
            device_id={"gx": lax.rem(me + s, count_gx)}, device_id_type=MESH)

    def b_own(i):
        return pltpu.make_async_copy(
            second.at[pl.ds(me * rows_x + i * STEP, STEP)],
            late.at[pl.ds(i * STEP, STEP), pl.ds(me * cols, cols)], b_send.at[i, 0])

    def z_part(n, s, source):
        slot = lax.rem(n, slots)
        r, i = n // steps, lax.rem(n, steps)
        return pltpu.make_async_remote_copy(
            src_ref=planes.at[slot, :, pl.ds(lax.rem(my + s, count_gy) * rows_y, rows_y)],
            dst_ref=result.at[r, source, pl.ds(i * STEP, STEP)],
            send_sem=z_send.at[n, s], recv_sem=z_recv.at[n, s],
            device_id={"gy": lax.rem(my + s, count_gy)}, device_id_type=MESH)

    def z_own(n):
        slot = lax.rem(n, slots)
        r, i = n // steps, lax.rem(n, steps)
        return pltpu.make_async_copy(
            planes.at[slot, :, pl.ds(my * rows_y, rows_y)],
            result.at[r, my, pl.ds(i * STEP, STEP)], z_send.at[n, 0])

    load(0).start()
    greet(count_gx, count_gy, me, my)

    kx = lax.broadcasted_iota(jnp.int32, (mid, lanes), 0)
    top = kx == 0
    kx_sq = (kx * kx).astype(jnp.float32)
    lane = lax.broadcasted_iota(jnp.int32, (mid, lanes), 1)
    kz = my * (lanes // 2) + jnp.where(lane < lanes // 2, lane, lane - lanes // 2)
    kz = jnp.where((kz == 0) & (lane >= lanes // 2), mid, kz)
    kz_sq = (kz * kz).astype(jnp.float32)
    far_sq = jnp.where(top, float(mid) ** 2, kx_sq)

    second_rows = second.reshape(length * cols, lanes)

    def along_x(c, _):
        @pl.when(c + 1 < pieces)
        def _():
            load(c + 1).start()
        load(c).wait()
        source = loaded.at[lax.rem(c, 2)].reshape(length * PIECE, lanes)
        target = first.at[c].reshape(length * PIECE, lanes)

        def pair(j, _):
            columns = [source[pl.ds(2 * j + k, length, stride=PIECE), :] for k in range(2)]
            spectrum = product(fwd_x[...], columns)
            freq = me * (cols // 2) + c * (PIECE // 2) + j
            sine_freq = jnp.where(freq == 0, mid, freq)
            plain = [(freq * freq).astype(jnp.float32), (sine_freq * sine_freq).astype(jnp.float32)]
            for r in range(2):
                scale = scales[r]
                weighted = []
                common = window(kx_sq + plain[0] + kz_sq, scale)
                weights = []
                for k in range(2):
                    edge = window(float(mid) ** 2 + plain[k] + kz_sq[:8], scale)
                    if k == 0:
                        cosine = common
                    else:
                        cosine = window(kx_sq + plain[1] + kz_sq, scale)
                    sine = jnp.concatenate([jnp.where(top[:8], edge, cosine[:8]), cosine[8:]], 0)
                    weighted.append(spectrum[k] * jnp.concatenate([cosine, sine], 0))
                out = product(inv_x[...], weighted)
                for k in range(2):
                    if r == 0:
                        target[pl.ds(2 * j + k, length, stride=PIECE), :] = out[k]
                    else:
                        second_rows[pl.ds(c * PIECE + 2 * j + k, length, stride=cols), :] = out[k]
            return 0

        lax.fori_loop(0, PIECE // 2, pair, 0)
        for s in range(1, count_gx):
            a_part(c, s, me).start()
        a_own(c).start()
        return 0

    lax.fori_loop(0, pieces, along_x, 0)

    def send_second(i, _):
        for s in range(1, count_gx):
            b_part(i, s, me).start()
        b_own(i).start()
        return 0

    lax.fori_loop(0, steps, send_second, 0)

    def along_y(n, bring):
        @pl.when(n >= slots)
        def _():
            for s in range(1, count_gy):
                z_part(n - slots, s, my).wait_send()
            z_own(n - slots).wait()
        bring.start()
        bring.wait()
        slot = lax.rem(n, slots)

        def pair(j, _):
            out = product(inv_y[...], [lines[2 * j], lines[2 * j + 1]])
            planes[slot, 2 * j] = out[0]
            planes[slot, 2 * j + 1] = out[1]
            return 0

        lax.fori_loop(0, STEP // 2, pair, 0)
        for s in range(1, count_gy):
            z_part(n, s, my).start()
        z_own(n).start()

    def wait_first(c, _):
        for s in range(1, count_gx):
            a_part(c, s, lax.rem(me + count_gx - s, count_gx)).wait_recv()
        a_own(c).wait()
        return 0

    lax.fori_loop(0, pieces, wait_first, 0)

    def first_rows(i, _):
        along_y(i, pltpu.make_async_copy(early.at[pl.ds(i * STEP, STEP)], lines, line_sem))
        return 0

    lax.fori_loop(0, steps, first_rows, 0)

    def later_rows(i, _):
        for s in range(1, count_gx):
            b_part(i, s, lax.rem(me + count_gx - s, count_gx)).wait_recv()
        b_own(i).wait()
        along_y(steps + i, pltpu.make_async_copy(late.at[pl.ds(i * STEP, STEP)], lines, line_sem))
        return 0

    lax.fori_loop(0, steps, later_rows, 0)

    def drain_a(c, _):
        for s in range(1, count_gx):
            a_part(c, s, me).wait_send()
        return 0

    lax.fori_loop(0, pieces, drain_a, 0)

    def drain_b(i, _):
        for s in range(1, count_gx):
            b_part(i, s, me).wait_send()
        return 0

    lax.fori_loop(0, steps, drain_b, 0)

    def drain_sends(n, _):
        for s in range(1, count_gy):
            z_part(n, s, my).wait_send()
        z_own(n).wait()
        return 0

    lax.fori_loop(max(0, 2 * steps - slots), 2 * steps, drain_sends, 0)

    def drain_z(n, _):
        for s in range(1, count_gy):
            z_part(n, s, lax.rem(my + count_gy - s, count_gy)).wait_recv()
        return 0

    lax.fori_loop(0, 2 * steps, drain_z, 0)


def per_device(density, radius_cells):
    rows_x, rows_y, length = density.shape
    count_gx = lax.axis_size("gx")
    count_gy = lax.axis_size("gy")
    lanes = length // count_gy
    cols = length // count_gx
    steps = rows_x // STEP
    f32 = jnp.float32
    vmem = pl.BlockSpec(memory_space=pltpu.VMEM)
    hbm = pl.BlockSpec(memory_space=pl.ANY)
    dma = pltpu.SemaphoreType.DMA

    table_z, gain_z = basis(length, blocked(length, count_gy))
    table_y, gain_y = basis(length, paired(length))
    table_x, gain_x = basis(length, blocked(length, 1))
    flops = 2 * 3 * rows_x * rows_y * length * length

    cube = pl.pallas_call(
        functools.partial(forward_kernel, count_gx, count_gy),
        out_shape=jax.ShapeDtypeStruct((length, cols, lanes), f32),
        in_specs=[hbm, vmem, vmem],
        out_specs=hbm,
        scratch_shapes=[
            pltpu.VMEM((2, STEP, rows_y, length), f32),
            pltpu.VMEM((steps, count_gy, STEP, rows_y, lanes), f32),
            pltpu.VMEM((rows_x, length, lanes), f32),
            pltpu.VMEM((rows_x, length, lanes), f32),
            dma((2,)), dma((steps, count_gy)), dma((steps, count_gy)),
            dma((steps, count_gx)), dma((steps, count_gx)),
        ],
        compiler_params=pltpu.CompilerParams(
            collective_id=0, has_side_effects=True, vmem_limit_bytes=VMEM),
        cost_estimate=pl.CostEstimate(flops=2 * flops, bytes_accessed=8 * density.size, transcendentals=0),
        name="forward",
    )(density, tripled(table_z.T, 0), tripled(table_y, 1))

    scales = 2.0 * math.pi / length * radius_cells.astype(f32)
    pieces = cols // PIECE
    slots = 4
    field = jax.ShapeDtypeStruct((rows_x, length, lanes), f32)
    _, _, fields = pl.pallas_call(
        functools.partial(inverse_kernel, count_gx, count_gy, rows_x, rows_y),
        out_shape=(field, field, jax.ShapeDtypeStruct((2, count_gy, rows_x, rows_y, lanes), f32)),
        in_specs=[pl.BlockSpec(memory_space=pltpu.SMEM), hbm, vmem, vmem, vmem],
        out_specs=(hbm, hbm, hbm),
        scratch_shapes=[
            pltpu.VMEM((2, length, PIECE, lanes), f32),
            pltpu.VMEM((pieces, length, PIECE, lanes), f32),
            pltpu.VMEM((length, cols, lanes), f32),
            pltpu.VMEM((STEP, length, lanes), f32),
            pltpu.VMEM((slots, STEP, length, lanes), f32),
            dma((2,)), dma((pieces, count_gx)), dma((pieces, count_gx)),
            dma((steps, count_gx)), dma((steps, count_gx)), dma(()),
            dma((2 * steps, count_gy)), dma((2 * steps, count_gy)),
        ],
        compiler_params=pltpu.CompilerParams(
            collective_id=1, has_side_effects=True, vmem_limit_bytes=VMEM),
        cost_estimate=pl.CostEstimate(flops=5 * flops, bytes_accessed=20 * density.size, transcendentals=0),
        name="inverse",
    )(scales * scales, cube, tripled(table_x, 1), tripled((table_x * gain_x).T, 1), tripled((table_y * gain_y).T, 1))

    inv_z = jnp.asarray(table_z * gain_z, f32).reshape(count_gy, lanes, length)
    return jnp.einsum("rgxyl,glz->rxyz", fields, inv_z,
                      precision=lax.Precision.HIGH, preferred_element_type=f32)


def solution(mesh):
    return jax.shard_map(
        per_device,
        mesh=mesh,
        in_specs=(P("gx", "gy", None), P()),
        out_specs=P(None, "gx", "gy", None),
        check_vma=False,
    )
```

```python
import functools
import math

import jax
import jax.numpy as jnp
import numpy as np
from jax import lax
from jax.experimental import pallas as pl
from jax.experimental.pallas import tpu as pltpu
from jax.sharding import PartitionSpec as P

MESH = pl.DeviceIdType.MESH
STEP = 8
PIECE = 8
VMEM = 63 * 1024 * 1024


def window(k_squared, scale_squared):
    u_squared = k_squared * scale_squared
    u_value = jnp.sqrt(u_squared)
    is_small = u_value < 0.2
    safe = jnp.where(is_small, 1.0, u_value)
    turns = jnp.floor(safe * (1.0 / math.pi) + 0.5)
    rest = safe - turns * 3.140625
    rest = rest - turns * 9.67502593994140625e-4
    rest = rest - turns * 1.509957990978376432e-7
    s2 = rest * rest
    sin_v = rest * (1.0 + s2 * (-1.6666666666e-1 + s2 * (8.3333333e-3 + s2 * (
        -1.98412698e-4 + s2 * (2.75573192e-6 + s2 * -2.50521084e-8)))))
    cos_v = 1.0 + s2 * (-0.5 + s2 * (4.16666666e-2 + s2 * (-1.38888889e-3 + s2 * (
        2.48015873e-5 + s2 * (-2.75573192e-7 + s2 * 2.08767570e-9)))))
    half = turns * 0.5
    sign = jnp.where(half == jnp.floor(half), 3.0, -3.0)
    closed = sign * (sin_v - safe * cos_v) / (safe * safe * safe)
    series = 1.0 - u_squared / 10.0 + u_squared * u_squared / 280.0
    return jnp.where(is_small, series, closed)


def basis(length, order):
    freq = np.array([length // 2 if s and f == 0 else f for f, s in order])
    sine = np.array([s and f > 0 for f, s in order])
    angle = 2.0 * math.pi / length * (np.outer(freq, np.arange(length)) % length)
    table = np.where(sine[:, None], np.sin(angle), np.cos(angle))
    gain = np.where((freq == 0) | (freq == length // 2), 1.0, 2.0) / length
    return table, gain[:, None]


def blocked(length, parts):
    width = length // 2 // parts
    return [(p * width + j, s) for p in range(parts) for s in (0, 1) for j in range(width)]


def paired(length):
    return [(f, s) for f in range(length // 2) for s in (0, 1)]


def tripled(table, axis):
    table = jnp.asarray(table, jnp.float32)
    high = table.astype(jnp.bfloat16)
    low = (table - high.astype(jnp.float32)).astype(jnp.bfloat16)
    return jnp.concatenate([high, low, high], axis)


def split(values, axis):
    high = values.astype(jnp.bfloat16)
    low = (values - high.astype(jnp.float32)).astype(jnp.bfloat16)
    return jnp.concatenate([high, high, low], axis)


def product(matrix, columns):
    width = columns[0].shape[1]
    if width % 128:
        return [jnp.dot(matrix, split(c, 0), preferred_element_type=jnp.float32) for c in columns]
    out = jnp.dot(matrix, split(jnp.concatenate(columns, 1), 0), preferred_element_type=jnp.float32)
    return [out[:, i * width:(i + 1) * width] for i in range(len(columns))]


def group_columns(length, count_gx):
    cols = length // count_gx
    full = (cols * 5 // 8 + PIECE - 1) // PIECE * PIECE
    return full, 2 * (cols - full)


class Line:
    def __init__(self, count):
        self.count = count
        self.half = count // 2
        self.me = lax.axis_index("gx")
        self.side = self.me // self.half
        self.pos = self.place(self.side, self.me)
        self.inner = self.pos < self.half // 2

    def place(self, side, index):
        return side * (index - self.half) + (1 - side) * (self.half - 1 - index)

    def near(self, s):
        pos = lax.rem(self.pos + s, self.half)
        return pos, self.index(self.side, pos)

    def far(self, s):
        pos = lax.rem(self.pos + s, self.half)
        return pos, self.index(1 - self.side, pos)

    def index(self, side, pos):
        return side * (self.half + pos) + (1 - side) * (self.half - 1 - pos)


def greet(count_gx, count_gy, me, my):
    barrier = pltpu.get_barrier_semaphore()
    for s in range(1, count_gx):
        pl.semaphore_signal(barrier, inc=1, device_id={"gx": lax.rem(me + s, count_gx)}, device_id_type=MESH)
    for s in range(1, count_gy):
        pl.semaphore_signal(barrier, inc=1, device_id={"gy": lax.rem(my + s, count_gy)}, device_id_type=MESH)
    pl.semaphore_wait(barrier, count_gx + count_gy - 2)


def loop(low, high, body):
    def step(i, _):
        body(i)
        return 0
    lax.fori_loop(low, high, step, 0)


def remote(src, dst, send, recv, axis, target):
    return pltpu.make_async_remote_copy(
        src_ref=src, dst_ref=dst, send_sem=send, recv_sem=recv,
        device_id={axis: target}, device_id_type=MESH)


def forward_kernel(count_gx, count_gy, density, fwd_z, fwd_y, cube, loaded, packed, lines, planes,
                   load_sem, z_send, z_recv, near_send, near_recv, far_send, far_recv, own_sem):
    rows_x, rows_y, length = density.shape
    lanes = length // count_gy
    full, shared = group_columns(length, count_gx)
    steps = rows_x // STEP
    line = Line(count_gx)
    me, half = line.me, line.half
    my = lax.axis_index("gy")
    groups = ((0, full), (full, shared))

    def load(i):
        return pltpu.make_async_copy(
            density.at[pl.ds(i * STEP, STEP)], loaded.at[lax.rem(i, 2)], load_sem.at[lax.rem(i, 2)])

    def z_part(i, s, source):
        target = lax.rem(my + s, count_gy)
        return remote(packed.at[i, target], lines.at[pl.ds(i * STEP, STEP), pl.ds(source * rows_y, rows_y)],
                      z_send.at[i, s], z_recv.at[i, s], "gy", target)

    def z_own(i):
        return pltpu.make_async_copy(
            packed.at[i, my], lines.at[pl.ds(i * STEP, STEP), pl.ds(my * rows_y, rows_y)], z_send.at[i, 0])

    def columns(i, group, pos, index):
        start = index * full if group == 0 else count_gx * full + pos * shared
        return planes.at[pl.ds(i * STEP, STEP), pl.ds(start, groups[group][1])]

    def landing(i, group, source):
        return cube.at[pl.ds(source * rows_x + i * STEP, STEP), pl.ds(*groups[group])]

    def near_part(i, group, s, source):
        pos, index = line.near(s)
        return remote(columns(i, group, pos, index), landing(i, group, source),
                      near_send.at[i, group, s], near_recv.at[i, group, s], "gx", index)

    def far_part(i, group, s, source):
        pos, index = line.far(s)
        return remote(columns(i, group, pos, index), landing(i, group, source),
                      far_send.at[i, group, s], far_recv.at[i, group, s], "gx", index)

    def own_part(i, group):
        return pltpu.make_async_copy(columns(i, group, line.pos, me), landing(i, group, me), own_sem.at[i, group])

    def send_far(i):
        for group in range(2):
            for s in range(half):
                far_part(i, group, s, me).start()

    load(0).start()
    greet(count_gx, count_gy, me, my)

    def along_z(i):
        @pl.when(i + 1 < steps)
        def _():
            load(i + 1).start()
        load(i).wait()

        def pair(j):
            rows = loaded[lax.rem(i, 2), pl.ds(2 * j, 2)].reshape(2 * rows_y, length)
            out = jnp.dot(split(rows, 1), fwd_z[...], preferred_element_type=jnp.float32)
            for b in range(count_gy):
                packed[i, b, pl.ds(2 * j, 2)] = out[:, b * lanes:(b + 1) * lanes].reshape(2, rows_y, lanes)

        loop(0, STEP // 2, pair)
        for s in range(1, count_gy):
            z_part(i, s, my).start()
        z_own(i).start()

    loop(0, steps, along_z)

    def along_y(i):
        for s in range(1, count_gy):
            z_part(i, s, lax.rem(my + count_gy - s, count_gy)).wait_recv()
        z_own(i).wait()

        def pair(j):
            row = i * STEP + 2 * j
            out = product(fwd_y[...], [lines[row], lines[row + 1]])
            planes[row] = out[0]
            planes[row + 1] = out[1]

        loop(0, STEP // 2, pair)

        @pl.when(line.inner)
        def _():
            send_far(i)
        for group in range(2):
            for s in range(1, half):
                near_part(i, group, s, me).start()
            own_part(i, group).start()

    loop(0, steps, along_y)

    @pl.when(jnp.logical_not(line.inner))
    def _():
        loop(0, steps, send_far)

    def finish(i):
        for s in range(1, count_gy):
            z_part(i, s, my).wait_send()
        for group in range(2):
            for s in range(1, half):
                near_part(i, group, s, me).wait_send()
                source = line.index(line.side, lax.rem(line.pos + half - s, half))
                near_part(i, group, s, source).wait_recv()
            for s in range(half):
                far_part(i, group, s, me).wait_send()
                source = line.index(1 - line.side, lax.rem(line.pos + half - s, half))
                far_part(i, group, s, source).wait_recv()
            own_part(i, group).wait()

    loop(0, steps, finish)


def inverse_kernel(count_gx, count_gy, rows_x, rows_y, scales, cube, fwd_x, inv_x, inv_y,
                   early, late, result, loaded, weights, full_a, shared_a, full_b, shared_b, lines, planes,
                   load_sem, a_send, a_recv, a_own, s_send, s_recv, s_own, ac_send, ac_recv, ax_send, ax_recv,
                   b_send, b_recv, b_own, bf_send, bf_recv, line_sem, z_send, z_recv):
    length, _, lanes = cube.shape
    full, shared = group_columns(length, count_gx)
    count_f, count_s = full // PIECE, shared // PIECE
    steps = rows_x // STEP
    mid = length // 2
    line = Line(count_gx)
    me, half = line.me, line.half
    my = lax.axis_index("gy")
    slots = planes.shape[0]
    low = count_gx * full

    def load(group, c, slot):
        return pltpu.make_async_copy(
            cube.at[:, pl.ds((0 if group == 0 else full) + c * PIECE, PIECE)], loaded.at[slot], load_sem.at[slot])

    def rows_for(group, index, pos, i, size):
        start = index * rows_x if group == 0 else lax.rem(index, half) * rows_x
        return pl.ds(start + i, size)

    def place(group, source, c, size):
        start = source * full if group == 0 else low + line.place(line.side, source) * shared
        return pl.ds(start + c, size)

    def a_near(c, s, source):
        _, index = line.near(s)
        return remote(full_a.at[pl.ds(index * rows_x, rows_x), pl.ds(c * PIECE, PIECE)],
                      early.at[:, pl.ds(source * full + c * PIECE, PIECE)],
                      a_send.at[c, s], a_recv.at[c, s], "gx", index)

    def a_self(c):
        return pltpu.make_async_copy(
            full_a.at[pl.ds(me * rows_x, rows_x), pl.ds(c * PIECE, PIECE)],
            early.at[:, pl.ds(me * full + c * PIECE, PIECE)], a_own.at[c])

    def s_near(i, s, source):
        pos, index = line.near(s)
        return remote(shared_a.at[rows_for(1, index, pos, i * STEP, STEP)],
                      early.at[pl.ds(i * STEP, STEP), place(1, source, 0, shared)],
                      s_send.at[i, s], s_recv.at[i, s], "gx", index)

    def s_self(i):
        return pltpu.make_async_copy(
            shared_a.at[rows_for(1, me, line.pos, i * STEP, STEP)],
            early.at[pl.ds(i * STEP, STEP), place(1, me, 0, shared)], s_own.at[i])

    def a_far_columns(c, p, source, slot):
        index = line.index(1 - line.side, p)
        return remote(full_a.at[pl.ds(index * rows_x, rows_x), pl.ds(c * PIECE, PIECE)],
                      early.at[:, pl.ds(source * full + c * PIECE, PIECE)],
                      ac_send.at[c, p], ac_recv.at[c, slot], "gx", index)

    def a_far_rows(i, p, source, slot):
        index = line.index(1 - line.side, p)
        return remote(full_a.at[pl.ds(index * rows_x + i * STEP, STEP)],
                      early.at[pl.ds(i * STEP, STEP), pl.ds(source * full, full)],
                      ax_send.at[i, p], ax_recv.at[i, slot], "gx", index)

    def b_near(i, group, s, source):
        pos, index = line.near(s)
        store = full_b if group == 0 else shared_b
        return remote(store.at[rows_for(group, index, pos, i * STEP, STEP)],
                      late.at[pl.ds(i * STEP, STEP), place(group, source, 0, full if group == 0 else shared)],
                      b_send.at[i, group, s], b_recv.at[i, group, s], "gx", index)

    def b_self(i, group):
        store = full_b if group == 0 else shared_b
        return pltpu.make_async_copy(
            store.at[rows_for(group, me, line.pos, i * STEP, STEP)],
            late.at[pl.ds(i * STEP, STEP), place(group, me, 0, full if group == 0 else shared)], b_own.at[i, group])

    def b_far(i, s, source):
        _, index = line.far(s)
        return remote(full_b.at[pl.ds(index * rows_x + i * STEP, STEP)],
                      late.at[pl.ds(i * STEP, STEP), pl.ds(source * full, full)],
                      bf_send.at[i, s], bf_recv.at[i, s], "gx", index)

    def z_part(n, s, source):
        slot, r, i = lax.rem(n, slots), n // steps, lax.rem(n, steps)
        target = lax.rem(my + s, count_gy)
        return remote(planes.at[slot, :, pl.ds(target * rows_y, rows_y)],
                      result.at[r, source, pl.ds(i * STEP, STEP)],
                      z_send.at[n, s], z_recv.at[n, s], "gy", target)

    def z_own(n):
        slot, r, i = lax.rem(n, slots), n // steps, lax.rem(n, steps)
        return pltpu.make_async_copy(
            planes.at[slot, :, pl.ds(my * rows_y, rows_y)],
            result.at[r, my, pl.ds(i * STEP, STEP)], z_send.at[n, 0])

    load(0, 0, 0).start()
    greet(count_gx, count_gy, me, my)

    kx = lax.broadcasted_iota(jnp.int32, (mid, lanes), 0)
    top = lax.broadcasted_iota(jnp.int32, (8, lanes), 0) == 0
    kx_sq = (kx * kx).astype(jnp.float32)
    lane = lax.broadcasted_iota(jnp.int32, (1, lanes), 1)
    kz = my * (lanes // 2) + jnp.where(lane < lanes // 2, lane, lane - lanes // 2)
    kz = jnp.where((kz == 0) & (lane >= lanes // 2), mid, kz)
    kz_sq = (kz * kz).astype(jnp.float32)

    def along_x(r, group, c, slot):
        source = loaded.at[slot].reshape(length * PIECE, lanes)
        cols = full if group == 0 else shared
        outs = length if group == 0 else length // 2
        store = ((full_a, shared_a), (full_b, shared_b))[r][group].reshape(outs * cols, lanes)
        scale = scales[r]

        def weigh(k, ky_sq):
            cosine = window(kx_sq + (ky_sq + kz_sq), scale)
            edge = window(float(mid) ** 2 + ky_sq + jnp.broadcast_to(kz_sq, (8, lanes)), scale)
            weights[k, :mid] = cosine
            weights[k, mid:] = cosine
            weights[k, mid:mid + 8] = jnp.where(top, edge, cosine[:8])

        def pair(j):
            freq = c * (PIECE // 2) + j
            if group == 0:
                freq = me * (full // 2) + freq
            else:
                freq = low // 2 + line.pos * (shared // 2) + freq
            weigh(0, (freq * freq).astype(jnp.float32))

            @pl.when(freq == 0)
            def _():
                weigh(1, float(mid) ** 2)
            other = 1 - (freq + mid - 1) // mid
            columns = [source[pl.ds(2 * j + k, length, stride=PIECE), :] for k in range(2)]
            spectrum = product(fwd_x[...], columns)
            weighted = [spectrum[0] * weights[0], spectrum[1] * weights[other]]
            matrix = inv_x[...] if group == 0 else inv_x[pl.ds(line.side * outs, outs)]
            out = product(matrix, weighted)
            for k in range(2):
                store[pl.ds(c * PIECE + 2 * j + k, outs, stride=cols), :] = out[k]

        loop(0, PIECE // 2, pair)

    inner_places, outer_places = range(half // 2), range(half // 2, half)
    outer = jnp.logical_not(line.inner)

    def x_pass(r, sent):
        def full_piece(c):
            @pl.when(c + 1 < count_f)
            def _():
                load(0, c + 1, lax.rem(c + 1, 2)).start()

            @pl.when(c + 1 == count_f)
            def _():
                load(1, 0, count_f % 2).start()
            load(0, c, lax.rem(c, 2)).wait()
            along_x(r, 0, c, lax.rem(c, 2))
            if r == 0:
                @pl.when(line.inner)
                def _():
                    for p in inner_places:
                        a_far_columns(c, p, me, line.pos).start()
                for s in range(1, half):
                    a_near(c, s, me).start()
                a_self(c).start()

        loop(0, count_f, full_piece)
        sent()

        def shared_piece(c):
            @pl.when(c + 1 < count_s)
            def _():
                load(1, c + 1, lax.rem(count_f + c + 1, 2)).start()
            load(1, c, lax.rem(count_f + c, 2)).wait()
            along_x(r, 1, c, lax.rem(count_f + c, 2))

        loop(0, count_s, shared_piece)

    def inner_rows():
        @pl.when(line.inner)
        def _():
            def send(i):
                for p in outer_places:
                    a_far_rows(i, p, me, line.pos).start()
            loop(0, steps, send)

    x_pass(0, inner_rows)

    def send_rows(i):
        for s in range(1, half):
            s_near(i, s, me).start()
        s_self(i).start()

        @pl.when(outer)
        def _():
            for p in range(half):
                a_far_rows(i, p, me, line.pos).start()

    loop(0, steps, send_rows)
    load(0, 0, 0).start()
    x_pass(1, lambda: None)

    def along_y(n, bring):
        bring.start()

        @pl.when(n >= slots)
        def _():
            for s in range(1, count_gy):
                z_part(n - slots, s, my).wait_send()
            z_own(n - slots).wait()
        bring.wait()
        slot = lax.rem(n, slots)

        def pair(j):
            out = product(inv_y[...], [lines[2 * j], lines[2 * j + 1]])
            planes[slot, 2 * j] = out[0]
            planes[slot, 2 * j + 1] = out[1]

        loop(0, STEP // 2, pair)
        for s in range(1, count_gy):
            z_part(n, s, my).start()
        z_own(n).start()

    def near_source(s):
        return line.index(line.side, lax.rem(line.pos + half - s, half))

    def far_source(pos):
        return line.index(1 - line.side, pos)

    def send_b_near(i):
        for group in range(2):
            for s in range(1, half):
                b_near(i, group, s, me).start()
            b_self(i, group).start()

    def send_b_far(i):
        for s in range(half):
            b_far(i, s, me).start()

    batch = max(1, steps // 4)

    @pl.when(outer)
    def _():
        def send(n):
            loop(n * batch, (n + 1) * batch, send_b_near)
            loop(n * batch, (n + 1) * batch, send_b_far)
        loop(0, steps // batch, send)

    @pl.when(line.inner)
    def _():
        loop(0, steps, send_b_near)

    def wait_pieces(c):
        for s in range(1, half):
            a_near(c, s, near_source(s)).wait_recv()
        a_self(c).wait()

        @pl.when(line.inner)
        def _():
            for p in inner_places:
                a_far_columns(c, p, far_source(p), p).wait_recv()

    loop(0, count_f, wait_pieces)

    def first_rows(i):
        for s in range(1, half):
            s_near(i, s, near_source(s)).wait_recv()
        s_self(i).wait()
        for p in outer_places:
            a_far_rows(i, p, far_source(p), p).wait_recv()

        @pl.when(outer)
        def _():
            for p in inner_places:
                a_far_rows(i, p, far_source(p), p).wait_recv()

        @pl.when(jnp.logical_and(line.inner, i == steps - 1))
        def _():
            loop(0, batch, send_b_far)
        along_y(i, pltpu.make_async_copy(early.at[pl.ds(i * STEP, STEP)], lines, line_sem))

    loop(0, steps, first_rows)

    def later_rows(i):
        for group in range(2):
            for s in range(1, half):
                b_near(i, group, s, near_source(s)).wait_recv()
            b_self(i, group).wait()
        for s in range(half):
            b_far(i, s, far_source(lax.rem(line.pos + half - s, half))).wait_recv()

        @pl.when(jnp.logical_and(line.inner, jnp.logical_and(lax.rem(i + 1, batch) == 0, i + 1 < steps)))
        def _():
            loop(i + 1, i + 1 + batch, send_b_far)
        along_y(steps + i, pltpu.make_async_copy(late.at[pl.ds(i * STEP, STEP)], lines, line_sem))

    loop(0, steps, later_rows)

    def drain_a(c):
        for s in range(1, half):
            a_near(c, s, me).wait_send()

        @pl.when(line.inner)
        def _():
            for p in inner_places:
                a_far_columns(c, p, me, line.pos).wait_send()

    loop(0, count_f, drain_a)

    def drain_b(i):
        for s in range(1, half):
            s_near(i, s, me).wait_send()
        for p in outer_places:
            a_far_rows(i, p, me, line.pos).wait_send()

        @pl.when(outer)
        def _():
            for p in inner_places:
                a_far_rows(i, p, me, line.pos).wait_send()
        for group in range(2):
            for s in range(1, half):
                b_near(i, group, s, me).wait_send()
        for s in range(half):
            b_far(i, s, me).wait_send()

    loop(0, steps, drain_b)

    def drain_sends(n):
        for s in range(1, count_gy):
            z_part(n, s, my).wait_send()
        z_own(n).wait()

    loop(max(0, 2 * steps - slots), 2 * steps, drain_sends)

    def drain_z(n):
        for s in range(1, count_gy):
            z_part(n, s, lax.rem(my + count_gy - s, count_gy)).wait_recv()

    loop(0, 2 * steps, drain_z)


def per_device(density, radius_cells):
    rows_x, rows_y, length = density.shape
    count_gx = lax.axis_size("gx")
    count_gy = lax.axis_size("gy")
    half = count_gx // 2
    lanes = length // count_gy
    full, shared = group_columns(length, count_gx)
    count_f, count_s = full // PIECE, shared // PIECE
    steps = rows_x // STEP
    assert full % PIECE == 0 and shared % PIECE == 0
    f32 = jnp.float32
    vmem = pl.BlockSpec(memory_space=pltpu.VMEM)
    hbm = pl.BlockSpec(memory_space=pl.ANY)
    dma = pltpu.SemaphoreType.DMA

    table_z, gain_z = basis(length, blocked(length, count_gy))
    table_y, gain_y = basis(length, paired(length))
    table_x, gain_x = basis(length, blocked(length, 1))
    flops = 2 * 3 * rows_x * rows_y * length * length

    cube = pl.pallas_call(
        functools.partial(forward_kernel, count_gx, count_gy),
        out_shape=jax.ShapeDtypeStruct((length, full + shared, lanes), f32),
        in_specs=[hbm, vmem, vmem],
        out_specs=hbm,
        scratch_shapes=[
            pltpu.VMEM((2, STEP, rows_y, length), f32),
            pltpu.VMEM((steps, count_gy, STEP, rows_y, lanes), f32),
            pltpu.VMEM((rows_x, length, lanes), f32),
            pltpu.VMEM((rows_x, length, lanes), f32),
            dma((2,)), dma((steps, count_gy)), dma((steps, count_gy)),
            dma((steps, 2, half)), dma((steps, 2, half)),
            dma((steps, 2, half)), dma((steps, 2, half)), dma((steps, 2)),
        ],
        compiler_params=pltpu.CompilerParams(
            collective_id=0, has_side_effects=True, vmem_limit_bytes=VMEM),
        cost_estimate=pl.CostEstimate(flops=2 * flops, bytes_accessed=8 * density.size, transcendentals=0),
        name="forward",
    )(density, tripled(table_z.T, 0), tripled(table_y, 1))

    scales = 2.0 * math.pi / length * radius_cells.astype(f32)
    slots = 4
    field = jax.ShapeDtypeStruct((rows_x, length, lanes), f32)
    _, _, fields = pl.pallas_call(
        functools.partial(inverse_kernel, count_gx, count_gy, rows_x, rows_y),
        out_shape=(field, field, jax.ShapeDtypeStruct((2, count_gy, rows_x, rows_y, lanes), f32)),
        in_specs=[pl.BlockSpec(memory_space=pltpu.SMEM), hbm, vmem, vmem, vmem],
        out_specs=(hbm, hbm, hbm),
        scratch_shapes=[
            pltpu.VMEM((2, length, PIECE, lanes), f32),
            pltpu.VMEM((2, length, lanes), f32),
            pltpu.VMEM((length, full, lanes), f32),
            pltpu.VMEM((length // 2, shared, lanes), f32),
            pltpu.VMEM((length, full, lanes), f32),
            pltpu.VMEM((length // 2, shared, lanes), f32),
            pltpu.VMEM((STEP, length, lanes), f32),
            pltpu.VMEM((slots, STEP, length, lanes), f32),
            dma((2,)),
            dma((count_f, half)), dma((count_f, half)), dma((count_f,)),
            dma((steps, half)), dma((steps, half)), dma((steps,)),
            dma((count_f, half)), dma((count_f, half)),
            dma((steps, half)), dma((steps, half)),
            dma((steps, 2, half)), dma((steps, 2, half)), dma((steps, 2)),
            dma((steps, half)), dma((steps, half)),
            dma(()), dma((2 * steps, count_gy)), dma((2 * steps, count_gy)),
        ],
        compiler_params=pltpu.CompilerParams(
            collective_id=1, has_side_effects=True, vmem_limit_bytes=VMEM),
        cost_estimate=pl.CostEstimate(flops=5 * flops, bytes_accessed=20 * density.size, transcendentals=0),
        name="inverse",
    )(scales * scales, cube, tripled(table_x, 1), tripled((table_x * gain_x).T, 1),
      tripled((table_y * gain_y).T, 1))

    inv_z = jnp.asarray(table_z * gain_z, f32).reshape(count_gy, lanes, length)
    return jnp.einsum("rgxyl,glz->rxyz", fields, inv_z,
                      precision=lax.Precision.HIGH, preferred_element_type=f32)


def solution(mesh):
    return jax.shard_map(
        per_device,
        mesh=mesh,
        in_specs=(P("gx", "gy", None), P()),
        out_specs=P(None, "gx", "gy", None),
        check_vma=False,
    )
```

```python
import functools
import math

import jax
import jax.numpy as jnp
import numpy as np
from jax import lax
from jax.experimental import pallas as pl
from jax.experimental.pallas import tpu as pltpu
from jax.sharding import PartitionSpec as P

MESH = pl.DeviceIdType.MESH
STEP = 4
PIECE = 8
VMEM = 63 * 1024 * 1024


def window(k_squared, scale_squared):
    u_squared = k_squared * scale_squared
    u_value = jnp.sqrt(u_squared)
    is_small = u_value < 0.2
    safe = jnp.where(is_small, 1.0, u_value)
    turns = jnp.floor(safe * (1.0 / math.pi) + 0.5)
    rest = safe - turns * 3.140625
    rest = rest - turns * 9.67502593994140625e-4
    rest = rest - turns * 1.509957990978376432e-7
    s2 = rest * rest
    sin_v = rest * (1.0 + s2 * (-1.6666666666e-1 + s2 * (8.3333333e-3 + s2 * (
        -1.98412698e-4 + s2 * (2.75573192e-6 + s2 * -2.50521084e-8)))))
    cos_v = 1.0 + s2 * (-0.5 + s2 * (4.16666666e-2 + s2 * (-1.38888889e-3 + s2 * (
        2.48015873e-5 + s2 * (-2.75573192e-7 + s2 * 2.08767570e-9)))))
    half = turns * 0.5
    sign = jnp.where(half == jnp.floor(half), 3.0, -3.0)
    closed = sign * (sin_v - safe * cos_v) / (safe * safe * safe)
    series = 1.0 - u_squared / 10.0 + u_squared * u_squared / 280.0
    return jnp.where(is_small, series, closed)


def basis(length, order):
    freq = np.array([length // 2 if s and f == 0 else f for f, s in order])
    sine = np.array([s and f > 0 for f, s in order])
    angle = 2.0 * math.pi / length * (np.outer(freq, np.arange(length)) % length)
    table = np.where(sine[:, None], np.sin(angle), np.cos(angle))
    gain = np.where((freq == 0) | (freq == length // 2), 1.0, 2.0) / length
    return table, gain[:, None]


def blocked(length, parts):
    width = length // 2 // parts
    return [(p * width + j, s) for p in range(parts) for s in (0, 1) for j in range(width)]


def paired(length):
    return [(f, s) for f in range(length // 2) for s in (0, 1)]


def tripled(table, axis):
    table = jnp.asarray(table, jnp.float32)
    high = table.astype(jnp.bfloat16)
    low = (table - high.astype(jnp.float32)).astype(jnp.bfloat16)
    return jnp.concatenate([high, low, high], axis)


def split(values, axis):
    high = values.astype(jnp.bfloat16)
    low = (values - high.astype(jnp.float32)).astype(jnp.bfloat16)
    return jnp.concatenate([high, high, low], axis)


def product(matrix, columns):
    width = columns[0].shape[1]
    if width % 128:
        return [jnp.dot(matrix, split(c, 0), preferred_element_type=jnp.float32) for c in columns]
    out = jnp.dot(matrix, split(jnp.concatenate(columns, 1), 0), preferred_element_type=jnp.float32)
    return [out[:, i * width:(i + 1) * width] for i in range(len(columns))]


def group_columns(length, count_gx):
    cols = length // count_gx
    full = (cols * 5 // 8 + PIECE - 1) // PIECE * PIECE
    return full, 2 * (cols - full)


class Line:
    def __init__(self, count):
        self.count = count
        self.half = count // 2
        self.me = lax.axis_index("gx")
        self.side = self.me // self.half
        self.pos = self.place(self.side, self.me)
        self.inner = self.pos < self.half // 2

    def place(self, side, index):
        return side * (index - self.half) + (1 - side) * (self.half - 1 - index)

    def near(self, s):
        pos = lax.rem(self.pos + s, self.half)
        return pos, self.index(self.side, pos)

    def far(self, s):
        pos = lax.rem(self.pos + s, self.half)
        return pos, self.index(1 - self.side, pos)

    def index(self, side, pos):
        return side * (self.half + pos) + (1 - side) * (self.half - 1 - pos)


def greet(count_gx, count_gy, me, my):
    barrier = pltpu.get_barrier_semaphore()
    for s in range(1, count_gx):
        pl.semaphore_signal(barrier, inc=1, device_id={"gx": lax.rem(me + s, count_gx)}, device_id_type=MESH)
    for s in range(1, count_gy):
        pl.semaphore_signal(barrier, inc=1, device_id={"gy": lax.rem(my + s, count_gy)}, device_id_type=MESH)
    pl.semaphore_wait(barrier, count_gx + count_gy - 2)


def loop(low, high, body):
    def step(i, _):
        body(i)
        return 0
    lax.fori_loop(low, high, step, 0)


def remote(src, dst, send, recv, axis, target):
    return pltpu.make_async_remote_copy(
        src_ref=src, dst_ref=dst, send_sem=send, recv_sem=recv,
        device_id={axis: target}, device_id_type=MESH)


def forward_kernel(count_gx, count_gy, density, fwd_z, fwd_y, cube, loaded, packed, lines, planes,
                   load_sem, z_send, z_recv, near_send, near_recv, far_send, far_recv, own_sem):
    rows_x, rows_y, length = density.shape
    lanes = length // count_gy
    full, shared = group_columns(length, count_gx)
    steps = rows_x // STEP
    line = Line(count_gx)
    me, half = line.me, line.half
    my = lax.axis_index("gy")
    groups = ((0, full), (full, shared))

    def load(i):
        return pltpu.make_async_copy(
            density.at[pl.ds(i * STEP, STEP)], loaded.at[lax.rem(i, 2)], load_sem.at[lax.rem(i, 2)])

    def z_part(i, s, source):
        target = lax.rem(my + s, count_gy)
        return remote(packed.at[i, target], lines.at[pl.ds(i * STEP, STEP), pl.ds(source * rows_y, rows_y)],
                      z_send.at[i, s], z_recv.at[i, s], "gy", target)

    def z_own(i):
        return pltpu.make_async_copy(
            packed.at[i, my], lines.at[pl.ds(i * STEP, STEP), pl.ds(my * rows_y, rows_y)], z_send.at[i, 0])

    def columns(i, group, pos, index):
        start = index * full if group == 0 else count_gx * full + pos * shared
        return planes.at[pl.ds(i * STEP, STEP), pl.ds(start, groups[group][1])]

    def landing(i, group, source):
        return cube.at[pl.ds(source * rows_x + i * STEP, STEP), pl.ds(*groups[group])]

    def near_part(i, group, s, source):
        pos, index = line.near(s)
        return remote(columns(i, group, pos, index), landing(i, group, source),
                      near_send.at[i, group, s], near_recv.at[i, group, s], "gx", index)

    def far_part(i, group, s, source):
        pos, index = line.far(s)
        return remote(columns(i, group, pos, index), landing(i, group, source),
                      far_send.at[i, group, s], far_recv.at[i, group, s], "gx", index)

    def own_part(i, group):
        return pltpu.make_async_copy(columns(i, group, line.pos, me), landing(i, group, me), own_sem.at[i, group])

    def send_far(i):
        for group in range(2):
            for s in range(half):
                far_part(i, group, s, me).start()

    load(0).start()
    greet(count_gx, count_gy, me, my)

    def along_z(i):
        @pl.when(i + 1 < steps)
        def _():
            load(i + 1).start()
        load(i).wait()

        def pair(j):
            rows = loaded[lax.rem(i, 2), pl.ds(2 * j, 2)].reshape(2 * rows_y, length)
            out = jnp.dot(split(rows, 1), fwd_z[...], preferred_element_type=jnp.float32)
            for b in range(count_gy):
                packed[i, b, pl.ds(2 * j, 2)] = out[:, b * lanes:(b + 1) * lanes].reshape(2, rows_y, lanes)

        loop(0, STEP // 2, pair)
        for s in range(1, count_gy):
            z_part(i, s, my).start()
        z_own(i).start()

    lead = min(4, steps)
    loop(0, lead, along_z)

    def along_y(i):
        @pl.when(i + lead < steps)
        def _():
            along_z(i + lead)
        for s in range(1, count_gy):
            z_part(i, s, lax.rem(my + count_gy - s, count_gy)).wait_recv()
        z_own(i).wait()

        def pair(j):
            row = i * STEP + 2 * j
            out = product(fwd_y[...], [lines[row], lines[row + 1]])
            planes[row] = out[0]
            planes[row + 1] = out[1]

        loop(0, STEP // 2, pair)

        @pl.when(line.inner)
        def _():
            send_far(i)
        for group in range(2):
            for s in range(1, half):
                near_part(i, group, s, me).start()
            own_part(i, group).start()

    loop(0, steps, along_y)

    @pl.when(jnp.logical_not(line.inner))
    def _():
        loop(0, steps, send_far)

    def finish(i):
        for s in range(1, count_gy):
            z_part(i, s, my).wait_send()
        for group in range(2):
            for s in range(1, half):
                near_part(i, group, s, me).wait_send()
                source = line.index(line.side, lax.rem(line.pos + half - s, half))
                near_part(i, group, s, source).wait_recv()
            for s in range(half):
                far_part(i, group, s, me).wait_send()
                source = line.index(1 - line.side, lax.rem(line.pos + half - s, half))
                far_part(i, group, s, source).wait_recv()
            own_part(i, group).wait()

    loop(0, steps, finish)


def inverse_kernel(count_gx, count_gy, rows_x, rows_y, scales, cube, fwd_x, inv_x, inv_y,
                   early, late, result, loaded, weights, full_a, shared_a, full_b, shared_b, lines, planes,
                   load_sem, a_send, a_recv, a_own, c_send, c_recv, c_own, s_send, s_recv, s_own, ac_send, ac_recv, ax_send, ax_recv,
                   b_send, b_recv, b_own, bf_send, bf_recv, line_sem, z_send, z_recv):
    length, _, lanes = cube.shape
    full, shared = group_columns(length, count_gx)
    count_f, count_s = full // PIECE, shared // PIECE
    count_c = c_own.shape[0]
    steps = rows_x // STEP
    mid = length // 2
    line = Line(count_gx)
    me, half = line.me, line.half
    my = lax.axis_index("gy")
    slots = planes.shape[0]
    low = count_gx * full

    def load(group, c, slot):
        return pltpu.make_async_copy(
            cube.at[:, pl.ds((0 if group == 0 else full) + c * PIECE, PIECE)], loaded.at[slot], load_sem.at[slot])

    def rows_for(group, index, pos, i, size):
        start = index * rows_x if group == 0 else lax.rem(index, half) * rows_x
        return pl.ds(start + i, size)

    def place(group, source, c, size):
        start = source * full if group == 0 else low + line.place(line.side, source) * shared
        return pl.ds(start + c, size)

    def a_near(c, s, source):
        _, index = line.near(s)
        return remote(full_a.at[pl.ds(index * rows_x, rows_x), pl.ds(c * PIECE, PIECE)],
                      early.at[:, pl.ds(source * full + c * PIECE, PIECE)],
                      a_send.at[c, s], a_recv.at[c, s], "gx", index)

    def a_self(c):
        return pltpu.make_async_copy(
            full_a.at[pl.ds(me * rows_x, rows_x), pl.ds(c * PIECE, PIECE)],
            early.at[:, pl.ds(me * full + c * PIECE, PIECE)], a_own.at[c])

    def c_near(c, s, source):
        pos, index = line.near(s)
        return remote(shared_a.at[rows_for(1, index, pos, 0, rows_x), pl.ds(c * PIECE, PIECE)],
                      early.at[:, place(1, source, c * PIECE, PIECE)],
                      c_send.at[c, s], c_recv.at[c, s], "gx", index)

    def c_self(c):
        return pltpu.make_async_copy(
            shared_a.at[rows_for(1, me, line.pos, 0, rows_x), pl.ds(c * PIECE, PIECE)],
            early.at[:, place(1, me, c * PIECE, PIECE)], c_own.at[c])

    done = count_c * PIECE

    def s_near(i, s, source):
        pos, index = line.near(s)
        return remote(shared_a.at[rows_for(1, index, pos, i * STEP, STEP), pl.ds(done, shared - done)],
                      early.at[pl.ds(i * STEP, STEP), place(1, source, done, shared - done)],
                      s_send.at[i, s], s_recv.at[i, s], "gx", index)

    def s_self(i):
        return pltpu.make_async_copy(
            shared_a.at[rows_for(1, me, line.pos, i * STEP, STEP), pl.ds(done, shared - done)],
            early.at[pl.ds(i * STEP, STEP), place(1, me, done, shared - done)], s_own.at[i])

    def a_far_columns(c, p, source, slot):
        index = line.index(1 - line.side, p)
        return remote(full_a.at[pl.ds(index * rows_x, rows_x), pl.ds(c * PIECE, PIECE)],
                      early.at[:, pl.ds(source * full + c * PIECE, PIECE)],
                      ac_send.at[c, p], ac_recv.at[c, slot], "gx", index)

    def a_far_rows(i, p, source, slot):
        index = line.index(1 - line.side, p)
        return remote(full_a.at[pl.ds(index * rows_x + i * STEP, STEP)],
                      early.at[pl.ds(i * STEP, STEP), pl.ds(source * full, full)],
                      ax_send.at[i, p], ax_recv.at[i, slot], "gx", index)

    def b_near(i, group, s, source):
        pos, index = line.near(s)
        store = full_b if group == 0 else shared_b
        return remote(store.at[rows_for(group, index, pos, i * STEP, STEP)],
                      late.at[pl.ds(i * STEP, STEP), place(group, source, 0, full if group == 0 else shared)],
                      b_send.at[i, group, s], b_recv.at[i, group, s], "gx", index)

    def b_self(i, group):
        store = full_b if group == 0 else shared_b
        return pltpu.make_async_copy(
            store.at[rows_for(group, me, line.pos, i * STEP, STEP)],
            late.at[pl.ds(i * STEP, STEP), place(group, me, 0, full if group == 0 else shared)], b_own.at[i, group])

    def b_far(i, s, source):
        _, index = line.far(s)
        return remote(full_b.at[pl.ds(index * rows_x + i * STEP, STEP)],
                      late.at[pl.ds(i * STEP, STEP), pl.ds(source * full, full)],
                      bf_send.at[i, s], bf_recv.at[i, s], "gx", index)

    def z_part(n, s, source):
        slot, r, i = lax.rem(n, slots), n // steps, lax.rem(n, steps)
        target = lax.rem(my + s, count_gy)
        return remote(planes.at[slot, :, pl.ds(target * rows_y, rows_y)],
                      result.at[r, source, pl.ds(i * STEP, STEP)],
                      z_send.at[n, s], z_recv.at[n, s], "gy", target)

    def z_own(n):
        slot, r, i = lax.rem(n, slots), n // steps, lax.rem(n, steps)
        return pltpu.make_async_copy(
            planes.at[slot, :, pl.ds(my * rows_y, rows_y)],
            result.at[r, my, pl.ds(i * STEP, STEP)], z_send.at[n, 0])

    load(0, 0, 0).start()
    greet(count_gx, count_gy, me, my)

    kx = lax.broadcasted_iota(jnp.int32, (mid, lanes), 0)
    top = lax.broadcasted_iota(jnp.int32, (8, lanes), 0) == 0
    kx_sq = (kx * kx).astype(jnp.float32)
    lane = lax.broadcasted_iota(jnp.int32, (1, lanes), 1)
    kz = my * (lanes // 2) + jnp.where(lane < lanes // 2, lane, lane - lanes // 2)
    kz = jnp.where((kz == 0) & (lane >= lanes // 2), mid, kz)
    kz_sq = (kz * kz).astype(jnp.float32)

    def along_x(r, group, c, slot):
        source = loaded.at[slot].reshape(length * PIECE, lanes)
        cols = full if group == 0 else shared
        outs = length if group == 0 else length // 2
        store = ((full_a, shared_a), (full_b, shared_b))[r][group].reshape(outs * cols, lanes)
        scale = scales[r]

        def weigh(k, ky_sq):
            cosine = window(kx_sq + (ky_sq + kz_sq), scale)
            edge = window(float(mid) ** 2 + ky_sq + jnp.broadcast_to(kz_sq, (8, lanes)), scale)
            weights[k, :mid] = cosine
            weights[k, mid:] = cosine
            weights[k, mid:mid + 8] = jnp.where(top, edge, cosine[:8])

        def pair(j):
            freq = c * (PIECE // 2) + j
            if group == 0:
                freq = me * (full // 2) + freq
            else:
                freq = low // 2 + line.pos * (shared // 2) + freq
            weigh(0, (freq * freq).astype(jnp.float32))

            @pl.when(freq == 0)
            def _():
                weigh(1, float(mid) ** 2)
            other = 1 - (freq + mid - 1) // mid
            columns = [source[pl.ds(2 * j + k, length, stride=PIECE), :] for k in range(2)]
            spectrum = product(fwd_x[...], columns)
            weighted = [spectrum[0] * weights[0], spectrum[1] * weights[other]]
            matrix = inv_x[...] if group == 0 else inv_x[pl.ds(line.side * outs, outs)]
            out = product(matrix, weighted)
            for k in range(2):
                store[pl.ds(c * PIECE + 2 * j + k, outs, stride=cols), :] = out[k]

        loop(0, PIECE // 2, pair)

    inner_places, outer_places = range(half // 2), range(half // 2, half)
    outer = jnp.logical_not(line.inner)

    def x_pass(sent):
        def full_piece(c):
            @pl.when(c + 1 < count_f)
            def _():
                load(0, c + 1, lax.rem(c + 1, 2)).start()

            @pl.when(c + 1 == count_f)
            def _():
                load(1, 0, count_f % 2).start()
            load(0, c, lax.rem(c, 2)).wait()
            along_x(0, 0, c, lax.rem(c, 2))

            @pl.when(line.inner)
            def _():
                for p in inner_places:
                    a_far_columns(c, p, me, line.pos).start()
            for s in range(1, half):
                a_near(c, s, me).start()
            a_self(c).start()

        loop(0, count_f, full_piece)
        sent()

        def shared_piece(c):
            @pl.when(c + 1 < count_s)
            def _():
                load(1, c + 1, lax.rem(count_f + c + 1, 2)).start()
            load(1, c, lax.rem(count_f + c, 2)).wait()
            along_x(0, 1, c, lax.rem(count_f + c, 2))

            @pl.when(c < count_c)
            def _():
                for s in range(1, half):
                    c_near(c, s, me).start()
                c_self(c).start()

        loop(0, count_s, shared_piece)

    def inner_rows():
        @pl.when(line.inner)
        def _():
            def send(i):
                for p in outer_places:
                    a_far_rows(i, p, me, line.pos).start()
            loop(0, steps, send)

    x_pass(inner_rows)

    def send_rows(i):
        for s in range(1, half):
            s_near(i, s, me).start()
        s_self(i).start()

        @pl.when(outer)
        def _():
            for p in range(half):
                a_far_rows(i, p, me, line.pos).start()

    loop(0, steps, send_rows)
    load(0, 0, 0).start()

    def along_y(n, bring):
        bring.start()

        @pl.when(n >= slots)
        def _():
            for s in range(1, count_gy):
                z_part(n - slots, s, my).wait_send()
            z_own(n - slots).wait()
        bring.wait()
        slot = lax.rem(n, slots)

        def pair(j):
            out = product(inv_y[...], [lines[2 * j], lines[2 * j + 1]])
            planes[slot, 2 * j] = out[0]
            planes[slot, 2 * j + 1] = out[1]

        loop(0, STEP // 2, pair)
        for s in range(1, count_gy):
            z_part(n, s, my).start()
        z_own(n).start()

    def near_source(s):
        return line.index(line.side, lax.rem(line.pos + half - s, half))

    def far_source(pos):
        return line.index(1 - line.side, pos)

    def send_b_near(i):
        for group in range(2):
            for s in range(1, half):
                b_near(i, group, s, me).start()
            b_self(i, group).start()

    def send_b_far(i):
        for s in range(half):
            b_far(i, s, me).start()

    batch = max(1, steps // 8)

    def send_second():
        @pl.when(outer)
        def _():
            def send(n):
                loop(n * batch, (n + 1) * batch, send_b_near)
                loop(n * batch, (n + 1) * batch, send_b_far)
            loop(0, steps // batch, send)

        @pl.when(line.inner)
        def _():
            loop(0, steps, send_b_near)

    count = count_f + count_s

    def second_piece(n):
        slot = lax.rem(n, 2)

        @pl.when(n + 1 < count_f)
        def _():
            load(0, n + 1, 1 - slot).start()

        @pl.when(jnp.logical_and(n + 1 >= count_f, n + 1 < count))
        def _():
            load(1, n + 1 - count_f, 1 - slot).start()

        @pl.when(n < count_f)
        def _():
            load(0, n, slot).wait()
            along_x(1, 0, n, slot)

        @pl.when(n >= count_f)
        def _():
            load(1, n - count_f, slot).wait()
            along_x(1, 1, n - count_f, slot)

        @pl.when(n == count - 1)
        def _():
            send_second()

    def wait_pieces(c):
        for s in range(1, half):
            a_near(c, s, near_source(s)).wait_recv()
        a_self(c).wait()

        @pl.when(line.inner)
        def _():
            for p in inner_places:
                a_far_columns(c, p, far_source(p), p).wait_recv()

    def wait_shared(c):
        for s in range(1, half):
            c_near(c, s, near_source(s)).wait_recv()
        c_self(c).wait()

    def first_rows(i):
        @pl.when(i < count)
        def _():
            second_piece(i)

        @pl.when(i == 0)
        def _():
            loop(0, count_f, wait_pieces)
            loop(0, count_c, wait_shared)
        for s in range(1, half):
            s_near(i, s, near_source(s)).wait_recv()
        s_self(i).wait()
        for p in outer_places:
            a_far_rows(i, p, far_source(p), p).wait_recv()

        @pl.when(outer)
        def _():
            for p in inner_places:
                a_far_rows(i, p, far_source(p), p).wait_recv()

        @pl.when(jnp.logical_and(line.inner, i == steps - 1))
        def _():
            loop(0, batch, send_b_far)
        along_y(i, pltpu.make_async_copy(early.at[pl.ds(i * STEP, STEP)], lines, line_sem))

    loop(0, steps, first_rows)

    def later_rows(i):
        for group in range(2):
            for s in range(1, half):
                b_near(i, group, s, near_source(s)).wait_recv()
            b_self(i, group).wait()
        for s in range(half):
            b_far(i, s, far_source(lax.rem(line.pos + half - s, half))).wait_recv()

        @pl.when(jnp.logical_and(line.inner, jnp.logical_and(lax.rem(i + 1, batch) == 0, i + 1 < steps)))
        def _():
            loop(i + 1, i + 1 + batch, send_b_far)
        along_y(steps + i, pltpu.make_async_copy(late.at[pl.ds(i * STEP, STEP)], lines, line_sem))

    loop(0, steps, later_rows)

    def drain_a(c):
        for s in range(1, half):
            a_near(c, s, me).wait_send()

        @pl.when(line.inner)
        def _():
            for p in inner_places:
                a_far_columns(c, p, me, line.pos).wait_send()

    loop(0, count_f, drain_a)

    def drain_c(c):
        for s in range(1, half):
            c_near(c, s, me).wait_send()

    loop(0, count_c, drain_c)

    def drain_b(i):
        for s in range(1, half):
            s_near(i, s, me).wait_send()
        for p in outer_places:
            a_far_rows(i, p, me, line.pos).wait_send()

        @pl.when(outer)
        def _():
            for p in inner_places:
                a_far_rows(i, p, me, line.pos).wait_send()
        for group in range(2):
            for s in range(1, half):
                b_near(i, group, s, me).wait_send()
        for s in range(half):
            b_far(i, s, me).wait_send()

    loop(0, steps, drain_b)

    def drain_sends(n):
        for s in range(1, count_gy):
            z_part(n, s, my).wait_send()
        z_own(n).wait()

    loop(max(0, 2 * steps - slots), 2 * steps, drain_sends)

    def drain_z(n):
        for s in range(1, count_gy):
            z_part(n, s, lax.rem(my + count_gy - s, count_gy)).wait_recv()

    loop(0, 2 * steps, drain_z)


def per_device(density, radius_cells):
    rows_x, rows_y, length = density.shape
    count_gx = lax.axis_size("gx")
    count_gy = lax.axis_size("gy")
    half = count_gx // 2
    lanes = length // count_gy
    full, shared = group_columns(length, count_gx)
    count_f, count_s = full // PIECE, shared // PIECE
    steps = rows_x // STEP
    count_c = max(1, count_s // 3)
    assert full % PIECE == 0 and shared % PIECE == 0 and count_f + count_s <= steps
    f32 = jnp.float32
    vmem = pl.BlockSpec(memory_space=pltpu.VMEM)
    hbm = pl.BlockSpec(memory_space=pl.ANY)
    dma = pltpu.SemaphoreType.DMA

    table_z, gain_z = basis(length, blocked(length, count_gy))
    table_y, gain_y = basis(length, paired(length))
    table_x, gain_x = basis(length, blocked(length, 1))
    flops = 2 * 3 * rows_x * rows_y * length * length

    cube = pl.pallas_call(
        functools.partial(forward_kernel, count_gx, count_gy),
        out_shape=jax.ShapeDtypeStruct((length, full + shared, lanes), f32),
        in_specs=[hbm, vmem, vmem],
        out_specs=hbm,
        scratch_shapes=[
            pltpu.VMEM((2, STEP, rows_y, length), f32),
            pltpu.VMEM((steps, count_gy, STEP, rows_y, lanes), f32),
            pltpu.VMEM((rows_x, length, lanes), f32),
            pltpu.VMEM((rows_x, length, lanes), f32),
            dma((2,)), dma((steps, count_gy)), dma((steps, count_gy)),
            dma((steps, 2, half)), dma((steps, 2, half)),
            dma((steps, 2, half)), dma((steps, 2, half)), dma((steps, 2)),
        ],
        compiler_params=pltpu.CompilerParams(
            collective_id=0, has_side_effects=True, vmem_limit_bytes=VMEM),
        cost_estimate=pl.CostEstimate(flops=2 * flops, bytes_accessed=8 * density.size, transcendentals=0),
        name="forward",
    )(density, tripled(table_z.T, 0), tripled(table_y, 1))

    scales = 2.0 * math.pi / length * radius_cells.astype(f32)
    slots = 8
    field = jax.ShapeDtypeStruct((rows_x, length, lanes), f32)
    _, _, fields = pl.pallas_call(
        functools.partial(inverse_kernel, count_gx, count_gy, rows_x, rows_y),
        out_shape=(field, field, jax.ShapeDtypeStruct((2, count_gy, rows_x, rows_y, lanes), f32)),
        in_specs=[pl.BlockSpec(memory_space=pltpu.SMEM), hbm, vmem, vmem, vmem],
        out_specs=(hbm, hbm, hbm),
        scratch_shapes=[
            pltpu.VMEM((2, length, PIECE, lanes), f32),
            pltpu.VMEM((2, length, lanes), f32),
            pltpu.VMEM((length, full, lanes), f32),
            pltpu.VMEM((length // 2, shared, lanes), f32),
            pltpu.VMEM((length, full, lanes), f32),
            pltpu.VMEM((length // 2, shared, lanes), f32),
            pltpu.VMEM((STEP, length, lanes), f32),
            pltpu.VMEM((slots, STEP, length, lanes), f32),
            dma((2,)),
            dma((count_f, half)), dma((count_f, half)), dma((count_f,)),
            dma((count_c, half)), dma((count_c, half)), dma((count_c,)),
            dma((steps, half)), dma((steps, half)), dma((steps,)),
            dma((count_f, half)), dma((count_f, half)),
            dma((steps, half)), dma((steps, half)),
            dma((steps, 2, half)), dma((steps, 2, half)), dma((steps, 2)),
            dma((steps, half)), dma((steps, half)),
            dma(()), dma((2 * steps, count_gy)), dma((2 * steps, count_gy)),
        ],
        compiler_params=pltpu.CompilerParams(
            collective_id=1, has_side_effects=True, vmem_limit_bytes=VMEM),
        cost_estimate=pl.CostEstimate(flops=5 * flops, bytes_accessed=20 * density.size, transcendentals=0),
        name="inverse",
    )(scales * scales, cube, tripled(table_x, 1), tripled((table_x * gain_x).T, 1),
      tripled((table_y * gain_y).T, 1))

    inv_z = jnp.asarray(table_z * gain_z, f32).reshape(count_gy, lanes, length)
    return jnp.einsum("rgxyl,glz->rxyz", fields, inv_z,
                      precision=lax.Precision.HIGH, preferred_element_type=f32)


def solution(mesh):
    return jax.shard_map(
        per_device,
        mesh=mesh,
        in_specs=(P("gx", "gy", None), P()),
        out_specs=P(None, "gx", "gy", None),
        check_vma=False,
    )
```
